32 devices in a mesh: seq: 8 (over z, core), ctx: 4 (over y, x).
Axes of the slice: x: 2, y: 2, z: 4, core: 2. Of those that a mesh axis runs over, the one named last changes fastest.
Arguments:
- queries: bfloat16 [8192, 2048], P(('seq', 'ctx')), parts along dimension 0, may hold values from -16 to 16
- key_rows: bfloat16 [8192, 512], P(('seq', 'ctx')), parts along dimension 0, may hold values from -16 to 16
- value_rows: bfloat16 [8192, 512], P(('seq', 'ctx')), parts along dimension 0, may hold values from -6 to 6
- doc_lengths: int32 [32], P('seq'), parts along dimension 0, may hold values from 1 to 512, 1024 in all
- block_owner: int32 [64], P('seq'), parts along dimension 0, may hold values from 0 to 7, as said below
Outputs:
- attended: bfloat16 [8192, 2048], P(('seq', 'ctx')), parts along dimension 0
The draws below stay inside these ranges and needn't reach their ends.
There are 8 independent parts, one for each index of `seq`. The reference program is written for one: setup_inputs(seed, part) draws one part's arguments, and reference() takes and returns one part's arrays. A program takes and returns all parts, laid end to end along the dimension named above; each array names one. Nothing has to cross between parts.
Inputs may be any that keep to these rules, and one draw needn't show every extreme that they name: `block_owner`: slots come in aligned groups of 4 blocks; each group holds exactly the blocks with the same group number, in some order.
All inputs are finite; a program needn't handle non-finite values.
Results may differ from the reference program's by a relative error of at most 0.0035.
Values may be sent and summed in bfloat16 or wider, within the bound.
A program may use at most 64 MiB of HBM per device.

```python
import math
import jax
import jax.numpy as jnp
import numpy as np
from jax import lax

Q_HEADS = 16
KV_HEADS = 4
HEAD_DIM = 128
BLOCK_ROWS = 128
TOK_DEV = 256
GROUP_SIZE = 4
TOKENS = 1024
BLOCKS_ALL = 8
DOC_COUNT = 4
DOC_MOST = 512


def drawn_draw(key, columns):
    return jnp.clip(jax.random.normal(key, (TOKENS, columns), jnp.float32), -6.0, 6.0)


def draw_queries(key, part):
    drawn = drawn_draw(jax.random.fold_in(key, 1), Q_HEADS * HEAD_DIM)
    return drawn.astype(jnp.bfloat16)


def draw_key_rows(key, part):
    drawn = drawn_draw(jax.random.fold_in(key, 2), KV_HEADS * HEAD_DIM)
    return drawn.astype(jnp.bfloat16)


def draw_block_owner(key, part):
    group_size = 2 * (TOK_DEV // BLOCK_ROWS)
    group_count = BLOCKS_ALL // group_size
    group_keys = jax.random.split(key, group_count)
    orders = jax.vmap(lambda one_key: jax.random.permutation(one_key, group_size))(group_keys)
    offsets = (jnp.arange(group_count, dtype=jnp.int32) * group_size)[:, None]
    return (orders.astype(jnp.int32) + offsets).reshape(BLOCKS_ALL)


def block_scale(rng, shape, shards, least, high):
    def one(position, shards_of):
        draws = jax.random.uniform(jax.random.fold_in(jax.random.fold_in(rng, 6), position), (shards_of,), jnp.float32, least / len(shards), high / len(shards))
        return jnp.repeat(jnp.exp(draws), shape[position] // shards_of).reshape((-1,) + (1,) * (len(shape) - position - 1))

    factor_of = one(*shards[0])
    for cut in shards[1:]:
        factor_of = factor_of * one(*cut)
    return factor_of


def split_up(count, total, limit, lean):
    loads = [(1 << 20) // math.isqrt(standing ** lean) + 1 for standing in range(2, count + 1)]
    spare, holding = total - limit - (count - 1), [1] * (count - 1)
    while spare > 0:
        movable = [i for i in range(count - 1) if holding[i] < limit]
        pool, budget = sum([loads[i] for i in movable]), spare
        for i in movable:
            addition = min(limit - holding[i], max(1, budget * loads[i] // pool), spare)
            holding[i] = holding[i] + addition
            spare = spare - addition
    return np.array([limit] + holding)


def uneven_parts(own_key, number_of, total, reach, slope):
    if number_of == 2:
        one = jax.random.randint(own_key, (), max(1, total - reach), min(reach, total - 1) + 1)
        return jnp.stack([one, total - one])
    sizes = jnp.asarray(split_up(number_of, total, reach, slope), jnp.int32)
    twos = (number_of - 1) // 2
    source_of, taker = sizes[1:1 + 2 * twos:2], sizes[2:2 + 2 * twos:2]
    room = jnp.minimum(source_of - 1, reach - taker)
    passed = jax.random.randint(jax.random.fold_in(own_key, 1), (twos,), 0, 1 << 20) % (room + 1)
    sizes = sizes.at[1:1 + 2 * twos:2].set(source_of - passed).at[2:2 + 2 * twos:2].set(taker + passed)
    return sizes[jax.random.permutation(jax.random.fold_in(own_key, 2), number_of)]


def normal_values(key, extent, scale, limit, pieces=(), held_as=jnp.bfloat16):
    entries = scale * jax.random.normal(key, extent, jnp.float32)
    if pieces:
        entries = entries * block_scale(key, extent, pieces, -0.22, 0.18)
    return jnp.clip(entries, -limit, limit).astype(held_as)


def setup_inputs(seed: int = 0, part: int = 0) -> dict:
    seeds = jax.random.split(jax.random.key(seed), 6)
    part_keys = jax.random.split(jax.random.fold_in(seeds[5], part), 6)
    queries = draw_queries(jax.random.fold_in(jax.random.fold_in(seeds[5], part), 71), part)
    key_rows = draw_key_rows(jax.random.fold_in(jax.random.fold_in(seeds[5], part), 71), part)
    value_rows = normal_values(part_keys[2], (TOKENS, KV_HEADS * HEAD_DIM), 1.0, 6.0, ((0, 4),))
    doc_lengths = uneven_parts(part_keys[3], DOC_COUNT, TOKENS, DOC_MOST, 1).astype(jnp.int32)
    block_owner = draw_block_owner(jax.random.fold_in(jax.random.fold_in(seeds[5], part), 71), part)
    return {"queries": queries, "key_rows": key_rows, "value_rows": value_rows, "doc_lengths": doc_lengths, "block_owner": block_owner}


NEGATIVE = -1.0e30


def reference(queries, key_rows, value_rows, doc_lengths, block_owner):
    slot_ids = jnp.arange(TOKENS, dtype=jnp.int32)
    places = block_owner[slot_ids // BLOCK_ROWS] * BLOCK_ROWS + slot_ids % BLOCK_ROWS
    doc_ends = jnp.cumsum(doc_lengths)
    documents = jnp.sum((places[:, None] >= doc_ends[None, :]).astype(jnp.int32), axis=1)
    key_heads = key_rows.astype(jnp.float32).reshape(TOKENS, KV_HEADS, HEAD_DIM)
    value_heads = value_rows.astype(jnp.float32).reshape(TOKENS, KV_HEADS, HEAD_DIM)
    block_size = min(512, TOKENS)
    scaling = HEAD_DIM ** -0.5

    def one_block(start):
        query_block = lax.dynamic_slice_in_dim(queries, start, block_size, 0).astype(jnp.float32)
        query_block = query_block.reshape(block_size, KV_HEADS, GROUP_SIZE, HEAD_DIM)
        query_places = lax.dynamic_slice_in_dim(places, start, block_size, 0)
        query_docs = lax.dynamic_slice_in_dim(documents, start, block_size, 0)
        allowed = (documents[None, :] == query_docs[:, None]) & (places[None, :] <= query_places[:, None])
        scores = jnp.einsum("rhgd,khd->hgrk", query_block, key_heads) * scaling
        scores = jnp.where(allowed[None, None], scores, NEGATIVE)
        largest = jnp.max(scores, axis=-1, keepdims=True)
        weights = jnp.where(allowed[None, None], jnp.exp(scores - largest), 0.0)
        totals = jnp.sum(weights, axis=-1)
        rounded = lax.optimization_barrier(weights.astype(jnp.bfloat16)).astype(jnp.float32)
        mixed = jnp.einsum("hgrk,khd->hgrd", rounded, value_heads) / totals[..., None]
        mixed = jnp.transpose(mixed, (2, 0, 1, 3)).reshape(block_size, Q_HEADS * HEAD_DIM)
        return mixed.astype(jnp.bfloat16)

    starts = jnp.arange(0, TOKENS, block_size, dtype=jnp.int32)
    return lax.map(one_block, starts).reshape(TOKENS, Q_HEADS * HEAD_DIM)
```

```python
import functools
import math

import jax
import jax.numpy as jnp
from jax import lax
from jax.experimental import pallas as pl
from jax.experimental.pallas import tpu as pltpu
from jax.sharding import PartitionSpec as P

HEAD_DIM = 128
BLOCK_ROWS = 128
GROUP_SIZE = 4
NEGATIVE = -1e30
MESH = pl.DeviceIdType.MESH
EXPONENT = HEAD_DIM ** -0.5 * math.log2(math.e)

OWN, PARTNER, PREV, CROSS = range(4)


def kernel(
    devices, q_hbm, k_hbm, v_hbm, lengths_hbm, owner_hbm, out,
    lengths, owner, q, kbuf, vbuf, bias, scores, top, weights, total, acc,
    local_sem, send_sem, recv_sem,
):
    rows = q.shape[0]
    kv_heads = kbuf.shape[2] // HEAD_DIM
    half = rows // 2
    me = lax.axis_index("ctx")
    partner = me + 1 - 2 * (me % 2)
    prev = me - 2
    cross = partner - 2
    nxt = me + 2
    has_prev = me >= 2
    has_next = me < devices - 2

    barrier = pltpu.get_barrier_semaphore()

    def greet(device):
        pl.semaphore_signal(barrier, inc=1, device_id={"ctx": device}, device_id_type=MESH)

    greet(partner)
    pl.when(has_prev)(lambda: greet(prev))
    pl.when(has_next)(lambda: greet(nxt))

    local = [
        pltpu.make_async_copy(k_hbm, kbuf.at[OWN], local_sem.at[0]),
        pltpu.make_async_copy(v_hbm, vbuf.at[OWN], local_sem.at[1]),
        pltpu.make_async_copy(lengths_hbm, lengths, local_sem.at[2]),
        pltpu.make_async_copy(owner_hbm, owner, local_sem.at[3]),
        pltpu.make_async_copy(q_hbm, q, local_sem.at[4]),
    ]
    for copy in local:
        copy.start()
    pl.semaphore_wait(barrier, 1 + has_prev.astype(jnp.int32) + has_next.astype(jnp.int32))

    def column(head):
        return pl.ds(head * HEAD_DIM if isinstance(head, int) else pl.multiple_of(head * HEAD_DIM, HEAD_DIM), HEAD_DIM)

    part = [pl.ds(0, half), pl.ds(half, half)]

    def remote(source, target, index, device):
        return pltpu.make_async_remote_copy(
            src_ref=source, dst_ref=target, send_sem=send_sem.at[index],
            recv_sem=recv_sem.at[index], device_id={"ctx": device}, device_id_type=MESH,
        )

    def own_copy(hbm, buf, piece, chunk, index, device):
        return remote(hbm.at[part[piece]], buf.at[chunk, part[piece]], index, device)

    def relay(buf, chunk, piece, index, device):
        return remote(buf.at[chunk, part[piece]], buf.at[CROSS, part[piece]], index, device)

    k_partner = [own_copy(k_hbm, kbuf, i, PARTNER, i, partner) for i in (0, 1)]
    k_next = [own_copy(k_hbm, kbuf, i, PREV, 2 + i, nxt) for i in (0, 1)]
    k_to_next = relay(kbuf, PARTNER, 1, 4, nxt)
    k_to_partner = relay(kbuf, PREV, 0, 5, partner)
    v_first_partner = own_copy(v_hbm, vbuf, 1, PARTNER, 6, partner)
    v_first_next = own_copy(v_hbm, vbuf, 0, PREV, 7, nxt)

    def own_values(chunk, piece, g, index, device):
        view = part[piece], column(g)
        return remote(v_hbm.at[view], vbuf.at[(chunk, *view)], index + g, device)

    def relay_values(chunk, piece, g, index, device):
        view = part[piece], column(g)
        return remote(vbuf.at[(chunk, *view)], vbuf.at[(CROSS, *view)], index + g, device)

    def v_partner(g):
        return own_values(PARTNER, 0, g, 8, partner)

    def v_next(g):
        return own_values(PREV, 1, g, 8 + kv_heads, nxt)

    def v_to_next(g):
        return relay_values(PARTNER, 1, g, 8 + 2 * kv_heads, nxt)

    def v_to_partner(g):
        return relay_values(PREV, 0, g, 8 + 3 * kv_heads, partner)

    def start_all(copy_of):
        for g in range(kv_heads):
            copy_of(g).start()

    k_partner[1].start()
    pl.when(has_next)(lambda: k_next[0].start())
    k_partner[0].start()
    pl.when(has_next)(lambda: k_next[1].start())

    local[2].wait()
    local[3].wait()
    down = lax.broadcasted_iota(jnp.int32, (half, 1), 0)
    along = lax.broadcasted_iota(jnp.int32, (1, half), 1)

    def mask(chunk, device):
        for i in range(2):
            places = owner[2 * me + i] * BLOCK_ROWS + down
            end = lengths[0]
            starts = jnp.where(places >= end, end, 0)
            for d in range(1, lengths.shape[0]):
                end = end + lengths[d]
                starts = jnp.where(places >= end, end, starts)
            for j in range(2):
                keys = owner[2 * device + j] * BLOCK_ROWS + along
                allowed = (keys >= starts) & (keys <= places)
                bias[chunk, pl.ds(i * half, half), pl.ds(j * half, half)] = jnp.where(
                    allowed, 0.0, NEGATIVE
                )

    mask(OWN, me)
    mask(PARTNER, partner)

    @pl.when(has_prev)
    def _():
        mask(PREV, prev)
        mask(CROSS, cross)

    def score(chunk):
        @pl.loop(0, kv_heads, unroll=True)
        def _(g):
            keys = kbuf[chunk, :, column(g)]
            for j in range(GROUP_SIZE):
                h = g * GROUP_SIZE + j
                s = lax.dot_general(
                    q[:, column(h)], keys, (((1,), (1,)), ((), ())),
                    preferred_element_type=jnp.float32,
                )
                s = s + bias[chunk]
                scores[h, chunk] = s
                best = jnp.maximum(s[:, :half], s[:, half:])
                if chunk != OWN:
                    best = jnp.maximum(best, top[h])
                top[h] = best

    def weigh(g, chunks):
        own = vbuf[OWN, :, column(g)]
        for j in range(GROUP_SIZE):
            h = g * GROUP_SIZE + j
            largest = jnp.max(top[h], axis=1, keepdims=True)
            summed = jnp.zeros((rows, half), jnp.float32)
            for c in range(chunks):
                w = jnp.exp2((scores[h, c] - largest) * EXPONENT)
                summed = summed + (w[:, :half] + w[:, half:])
                weights[h, c] = w.astype(jnp.bfloat16)
            total[h] = jnp.sum(summed, axis=1, keepdims=True)
            acc[h] = jnp.dot(weights[h, OWN], own, preferred_element_type=jnp.float32)

    def mix(g):
        partners = vbuf[PARTNER, :, column(g)]
        prevs = vbuf[PREV, :, column(g)]
        for j in range(GROUP_SIZE):
            h = g * GROUP_SIZE + j
            acc[h] += jnp.dot(
                weights[h, PARTNER], partners, preferred_element_type=jnp.float32
            ) + jnp.dot(weights[h, PREV], prevs, preferred_element_type=jnp.float32)

    def finish(chunk):
        @pl.loop(0, kv_heads, unroll=True)
        def _(g):
            if chunk == CROSS:
                v_to_next(g).wait_recv()
                v_to_partner(g).wait_recv()
            values = vbuf[chunk, :, column(g)]
            for j in range(GROUP_SIZE):
                h = g * GROUP_SIZE + j
                mixed = acc[h] + jnp.dot(
                    weights[h, chunk], values, preferred_element_type=jnp.float32
                )
                out[:, column(h)] = (mixed * (1.0 / total[h])).astype(jnp.bfloat16)

    k_partner[1].wait_recv()
    pl.when(has_next)(k_to_next.start)

    @pl.when(has_prev)
    def _():
        k_next[0].wait_recv()
        k_to_partner.start()

    v_first_partner.start()

    @pl.when(has_next)
    def _():
        v_first_next.start()
        start_all(v_next)

    start_all(v_partner)
    local[0].wait()
    local[4].wait()
    score(OWN)
    k_partner[0].wait_recv()
    score(PARTNER)

    @pl.when(has_prev)
    def _():
        k_next[1].wait_recv()
        score(PREV)
        k_to_next.wait_recv()
        k_to_partner.wait_recv()
        score(CROSS)

    local[1].wait()
    middle = kv_heads // 2

    def weigh_all(first, last):
        for g in range(first, last):
            pl.when(has_prev)(lambda: weigh(g, 4))
            pl.when(jnp.logical_not(has_prev))(lambda: weigh(g, 2))

    weigh_all(0, middle)
    v_first_partner.wait_recv()
    pl.when(has_next)(lambda: start_all(v_to_next))

    @pl.when(has_prev)
    def _():
        v_first_next.wait_recv()
        start_all(v_to_partner)

    weigh_all(middle, kv_heads)
    for g in range(kv_heads):
        v_partner(g).wait_recv()

        @pl.when(has_prev)
        def _():
            v_next(g).wait_recv()
            mix(g)

    pl.when(has_prev)(lambda: finish(CROSS))
    pl.when(jnp.logical_not(has_prev))(lambda: finish(PARTNER))

    for copy in k_partner + [v_first_partner] + [v_partner(g) for g in range(kv_heads)]:
        copy.wait_send()

    @pl.when(has_next)
    def _():
        for copy in k_next + [k_to_next, v_first_next]:
            copy.wait_send()
        for g in range(kv_heads):
            v_next(g).wait_send()
            v_to_next(g).wait_send()

    @pl.when(has_prev)
    def _():
        k_to_partner.wait_send()
        for g in range(kv_heads):
            v_to_partner(g).wait_send()


def body(devices, queries, key_rows, value_rows, doc_lengths, block_owner):
    rows, width = queries.shape
    kv_width = key_rows.shape[1]
    heads, kv_heads = width // HEAD_DIM, kv_width // HEAD_DIM
    half = rows // 2
    return pl.pallas_call(
        functools.partial(kernel, devices),
        out_shape=pltpu.VMEM((rows, width), jnp.bfloat16),
        in_specs=[pl.BlockSpec(memory_space=pl.ANY)] * 5,
        out_specs=pl.BlockSpec(memory_space=pltpu.VMEM),
        scratch_shapes=[
            pltpu.SMEM(doc_lengths.shape, jnp.int32),
            pltpu.SMEM(block_owner.shape, jnp.int32),
            pltpu.VMEM((rows, width), jnp.bfloat16),
            pltpu.VMEM((4, rows, kv_width), jnp.bfloat16),
            pltpu.VMEM((4, rows, kv_width), jnp.bfloat16),
            pltpu.VMEM((4, rows, rows), jnp.float32),
            pltpu.VMEM((heads, 4, rows, rows), jnp.float32),
            pltpu.VMEM((heads, rows, half), jnp.float32),
            pltpu.VMEM((heads, 4, rows, rows), jnp.bfloat16),
            pltpu.VMEM((heads, rows, 1), jnp.float32),
            pltpu.VMEM((heads, rows, HEAD_DIM), jnp.float32),
            pltpu.SemaphoreType.DMA((5,)),
            pltpu.SemaphoreType.DMA((8 + 4 * kv_heads,)),
            pltpu.SemaphoreType.DMA((8 + 4 * kv_heads,)),
        ],
        compiler_params=pltpu.CompilerParams(
            collective_id=0, has_side_effects=True, vmem_limit_bytes=56 * 1024 * 1024
        ),
        name="attend",
    )(queries, key_rows, value_rows, doc_lengths, block_owner)


def solution(mesh):
    rows = P(("seq", "ctx"), None)
    return jax.shard_map(
        functools.partial(body, mesh.shape["ctx"]),
        mesh=mesh,
        in_specs=(rows, rows, rows, P("seq"), P("seq")),
        out_specs=rows,
        check_vma=False,
    )
```

```python
import functools
import itertools
import math

import jax
import jax.numpy as jnp
from jax import lax
from jax.experimental import pallas as pl
from jax.experimental.pallas import tpu as pltpu
from jax.sharding import PartitionSpec as P

HEAD_DIM = 128
BLOCK_ROWS = 128
GROUP_SIZE = 4
NEGATIVE = -1e30
MESH = pl.DeviceIdType.MESH
EXPONENT = HEAD_DIM ** -0.5 * math.log2(math.e)

OWN, PARTNER, PREV, CROSS = range(4)


def kernel(
    devices, q_hbm, k_hbm, v_hbm, lengths_hbm, owner_hbm, out,
    lengths, owner, q, kbuf, vbuf, bias, scores, top, weights, total, acc,
    q_far, k_far, v_far, far_bias, far_scores, far_weights, o_far,
    local_sem, send_sem, recv_sem, ready,
):
    rows = q.shape[0]
    kv_heads = kbuf.shape[2] // HEAD_DIM
    lent = kv_heads - 1
    half = rows // 2
    me = lax.axis_index("ctx")
    partner = me + 1 - 2 * (me % 2)
    prev = me - 2
    cross = partner - 2
    nxt = me + 2
    has_prev = me >= 2
    has_next = me < devices - 2
    no_prev = jnp.logical_not(has_prev)
    no_next = jnp.logical_not(has_next)
    whole = jnp.logical_or(has_next, no_prev)

    barrier = pltpu.get_barrier_semaphore()

    def greet(device):
        pl.semaphore_signal(barrier, inc=1, device_id={"ctx": device}, device_id_type=MESH)

    even = me % 2 == 0
    greet(partner)
    pl.when(jnp.logical_and(has_prev, even))(lambda: greet(prev))
    pl.when(has_next)(lambda: greet(nxt))

    local = [
        pltpu.make_async_copy(k_hbm, kbuf.at[OWN], local_sem.at[0]),
        pltpu.make_async_copy(v_hbm, vbuf.at[OWN], local_sem.at[1]),
        pltpu.make_async_copy(lengths_hbm, lengths, local_sem.at[2]),
        pltpu.make_async_copy(owner_hbm, owner, local_sem.at[3]),
        pltpu.make_async_copy(q_hbm, q, local_sem.at[4]),
    ]
    for copy in local:
        copy.start()
    below = jnp.logical_and(has_next, even).astype(jnp.int32)
    pl.semaphore_wait(barrier, 1 + has_prev.astype(jnp.int32) + below)

    @pl.when(jnp.logical_and(has_prev, jnp.logical_not(even)))
    def _():
        pl.semaphore_signal(ready, inc=1, device_id={"ctx": prev}, device_id_type=MESH)


    def column(head):
        return pl.ds(head * HEAD_DIM, HEAD_DIM)

    part = [pl.ds(0, half), pl.ds(half, half)]
    every = pl.ds(0, rows)
    rest = pl.ds(0, lent * HEAD_DIM)
    indices = itertools.count()

    def remote(source, target, device):
        index = next(indices)
        return pltpu.make_async_remote_copy(
            src_ref=source, dst_ref=target, send_sem=send_sem.at[index],
            recv_sem=recv_sem.at[index], device_id={"ctx": device}, device_id_type=MESH,
        )

    def own_copy(hbm, buf, piece, columns, chunk, device):
        return remote(hbm.at[piece, columns], buf.at[chunk, piece, columns], device)

    def relay(buf, chunk, piece, columns, device):
        return remote(buf.at[chunk, piece, columns], buf.at[CROSS, piece, columns], device)

    others = range(lent)
    straight = range(lent - 1)
    k_partner = [own_copy(k_hbm, kbuf, p, rest, PARTNER, partner) for p in part]
    k_next = [own_copy(k_hbm, kbuf, p, rest, PREV, nxt) for p in part]
    lent_partner = [
        own_copy(k_hbm, kbuf, every, column(lent), PARTNER, partner),
        own_copy(v_hbm, vbuf, every, column(lent), PARTNER, partner),
    ]
    v_first_partner = own_copy(v_hbm, vbuf, part[1], rest, PARTNER, partner)
    v_first_next = own_copy(v_hbm, vbuf, part[0], rest, PREV, nxt)
    v_partner = [own_copy(v_hbm, vbuf, part[0], column(g), PARTNER, partner) for g in others]
    v_next = [own_copy(v_hbm, vbuf, part[1], column(g), PREV, nxt) for g in others]
    k_to_next = [relay(kbuf, PARTNER, part[1], column(g), nxt) for g in straight]
    k_to_partner = [relay(kbuf, PREV, part[0], column(g), partner) for g in others]
    k_late = relay(kbuf, PREV, part[1], column(lent - 1), partner)
    v_to_partner = [relay(vbuf, PREV, part[0], column(g), partner) for g in others]
    v_late = [relay(vbuf, PREV, part[1], column(g), partner) for g in others]
    far_down = [
        remote(k_hbm.at[every, column(lent)], k_far.at[0], prev),
        remote(v_hbm.at[every, column(lent)], v_far.at[0], prev),
    ]
    far_across = [
        remote(k_far.at[0], k_far.at[1], partner),
        remote(v_far.at[0], v_far.at[1], partner),
    ]
    group = range(GROUP_SIZE)
    q_down = [
        remote(q_hbm.at[every, column(lent * GROUP_SIZE + j)], q_far.at[every, column(j)], prev)
        for j in group
    ]
    o_up = [
        remote(o_far.at[j], out.at[every, column(lent * GROUP_SIZE + j)], nxt) for j in group
    ]

    def start_all(copies):
        for copy in copies:
            copy.start()

    def receive_all(copies):
        for copy in copies:
            copy.wait_recv()

    def sent_all(copies):
        for copy in copies:
            copy.wait_send()

    k_partner[1].start()
    pl.when(whole)(lambda: start_all(lent_partner))
    pl.when(jnp.logical_and(has_next, jnp.logical_not(even)))(lambda: pl.semaphore_wait(ready, 1))

    @pl.when(has_next)
    def _():
        k_next[0].start()
        k_next[1].start()
        v_first_next.start()

    @pl.when(has_prev)
    def _():
        start_all(far_down)
        start_all(q_down)

    @pl.when(no_next)
    def _():
        k_partner[0].start()
        v_first_partner.start()

    local[2].wait()
    local[3].wait()
    down = lax.broadcasted_iota(jnp.int32, (half, 1), 0)
    along = lax.broadcasted_iota(jnp.int32, (1, half), 1)

    def mask(target, chunk, querier, device):
        for i in range(2):
            places = owner[2 * querier + i] * BLOCK_ROWS + down
            end = lengths[0]
            starts = jnp.where(places >= end, end, 0)
            for d in range(1, lengths.shape[0]):
                end = end + lengths[d]
                starts = jnp.where(places >= end, end, starts)
            for j in range(2):
                keys = owner[2 * device + j] * BLOCK_ROWS + along
                allowed = (keys >= starts) & (keys <= places)
                target[chunk, pl.ds(i * half, half), pl.ds(j * half, half)] = jnp.where(
                    allowed, 0.0, NEGATIVE
                )

    mask(bias, OWN, me, me)
    mask(bias, PARTNER, me, partner)

    @pl.when(has_prev)
    def _():
        mask(bias, PREV, me, prev)
        mask(bias, CROSS, me, cross)

    @pl.when(has_next)
    def _():
        mask(far_bias, 0, nxt, me)
        mask(far_bias, 1, nxt, partner)
        mask(far_bias, 2, nxt, nxt)
        mask(far_bias, 3, nxt, partner + 2)

    def attend(queries, keys, allowed):
        s = lax.dot_general(
            queries, keys, (((1,), (1,)), ((), ())), preferred_element_type=jnp.float32
        )
        return s + allowed

    def score(chunk, first, last):
        for g in range(first, last):
            keys = kbuf[chunk, :, column(g)]
            for j in group:
                h = g * GROUP_SIZE + j
                s = attend(q[:, column(h)], keys, bias[chunk])
                scores[h, chunk] = s
                best = jnp.maximum(s[:, :half], s[:, half:])
                if chunk != OWN:
                    best = jnp.maximum(best, top[h])
                top[h] = best

    def weigh(g, chunks):
        own = vbuf[OWN, :, column(g)]
        for j in group:
            h = g * GROUP_SIZE + j
            largest = jnp.max(top[h], axis=1, keepdims=True)
            summed = jnp.zeros((rows, half), jnp.float32)
            for c in range(chunks):
                w = jnp.exp2((scores[h, c] - largest) * EXPONENT)
                summed = summed + (w[:, :half] + w[:, half:])
                weights[h, c] = w.astype(jnp.bfloat16)
            total[h] = jnp.sum(summed, axis=1, keepdims=True)
            acc[h] = jnp.dot(weights[h, OWN], own, preferred_element_type=jnp.float32)

    def mix(g):
        partners = vbuf[PARTNER, :, column(g)]
        prevs = vbuf[PREV, :, column(g)]
        for j in group:
            h = g * GROUP_SIZE + j
            acc[h] += jnp.dot(
                weights[h, PARTNER], partners, preferred_element_type=jnp.float32
            ) + jnp.dot(weights[h, PREV], prevs, preferred_element_type=jnp.float32)

    def finish(chunk, g):
        values = vbuf[chunk, :, column(g)]
        for j in group:
            h = g * GROUP_SIZE + j
            mixed = acc[h] + jnp.dot(
                weights[h, chunk], values, preferred_element_type=jnp.float32
            )
            out[:, column(h)] = (mixed * (1.0 / total[h])).astype(jnp.bfloat16)

    def far_keys(c):
        return kbuf[c, :, column(lent)] if c < 2 else k_far[c - 2]

    def far_values(c):
        return vbuf[c, :, column(lent)] if c < 2 else v_far[c - 2]

    def far_score(j):
        q_down[j].wait_recv()
        for c in range(4):
            far_scores[j, c] = attend(q_far[:, column(j)], far_keys(c), far_bias[c])

    def far_finish(j):
        best = far_scores[j, 0]
        for c in range(1, 4):
            best = jnp.maximum(best, far_scores[j, c])
        largest = jnp.max(best, axis=1, keepdims=True)
        summed = jnp.zeros((rows, half), jnp.float32)
        for c in range(4):
            w = jnp.exp2((far_scores[j, c] - largest) * EXPONENT)
            summed = summed + (w[:, :half] + w[:, half:])
            far_weights[j, c] = w.astype(jnp.bfloat16)
        mixed = jnp.dot(far_weights[j, 0], far_values(0), preferred_element_type=jnp.float32)
        for c in range(1, 4):
            mixed += jnp.dot(far_weights[j, c], far_values(c), preferred_element_type=jnp.float32)
        share = 1.0 / jnp.sum(summed, axis=1, keepdims=True)
        o_far[j] = (mixed * share).astype(jnp.bfloat16)
        o_up[j].start()

    @pl.when(has_next)
    def _():
        for down_copy, across_copy in zip(far_down, far_across):
            down_copy.wait_recv()
            across_copy.start()
        k_partner[0].start()

    k_partner[1].wait_recv()

    @pl.when(has_next)
    def _():
        start_all(k_to_next)
        start_all(v_next)
        v_first_partner.start()

    @pl.when(has_prev)
    def _():
        k_next[0].wait_recv()
        start_all(k_to_partner)
        k_next[1].wait_recv()
        k_late.start()

    start_all(v_partner)
    local[0].wait()
    local[1].wait()
    local[4].wait()
    score(OWN, 0, lent)
    pl.when(no_prev)(lambda: score(OWN, lent, kv_heads))
    pl.when(whole)(lambda: receive_all(lent_partner))

    @pl.when(has_next)
    def _():
        far_across[0].wait_recv()
        far_score(0)
        far_score(1)
        far_across[1].wait_recv()
        far_finish(0)
        far_finish(1)
        for j in group[2:]:
            far_score(j)
            far_finish(j)

    k_partner[0].wait_recv()
    score(PARTNER, 0, lent)

    @pl.when(no_prev)
    def _():
        score(PARTNER, lent, kv_heads)
        for g in range(kv_heads):
            weigh(g, 2)
        v_first_partner.wait_recv()
        for g in range(kv_heads):
            if g < lent:
                v_partner[g].wait_recv()
            finish(PARTNER, g)

    @pl.when(has_prev)
    def _():
        score(PREV, 0, lent)
        for g in others:
            k_to_partner[g].wait_recv()
            (k_to_next[g] if g < lent - 1 else k_late).wait_recv()
            score(CROSS, g, g + 1)
            weigh(g, 4)
            if g == 1:
                v_first_next.wait_recv()
                start_all(v_to_partner)
        v_first_partner.wait_recv()
        for g in others:
            v_next[g].wait_recv()
            v_late[g].start()
            v_partner[g].wait_recv()
            mix(g)
        for g in others:
            v_to_partner[g].wait_recv()
            v_late[g].wait_recv()
            finish(CROSS, g)
        receive_all(o_up)

    sent_all(k_partner + v_partner + [v_first_partner])
    pl.when(whole)(lambda: sent_all(lent_partner))
    pl.when(has_next)(
        lambda: sent_all(k_next + k_to_next + v_next + far_across + o_up + [v_first_next])
    )
    pl.when(has_prev)(
        lambda: sent_all(k_to_partner + v_to_partner + v_late + far_down + q_down + [k_late])
    )


def body(devices, queries, key_rows, value_rows, doc_lengths, block_owner):
    rows, width = queries.shape
    kv_width = key_rows.shape[1]
    heads, kv_heads = width // HEAD_DIM, kv_width // HEAD_DIM
    half = rows // 2
    copies = 8 * kv_heads + 4 + 2 * GROUP_SIZE
    return pl.pallas_call(
        functools.partial(kernel, devices),
        out_shape=pltpu.VMEM((rows, width), jnp.bfloat16),
        in_specs=[pl.BlockSpec(memory_space=pl.ANY)] * 5,
        out_specs=pl.BlockSpec(memory_space=pltpu.VMEM),
        scratch_shapes=[
            pltpu.SMEM(doc_lengths.shape, jnp.int32),
            pltpu.SMEM(block_owner.shape, jnp.int32),
            pltpu.VMEM((rows, width), jnp.bfloat16),
            pltpu.VMEM((4, rows, kv_width), jnp.bfloat16),
            pltpu.VMEM((4, rows, kv_width), jnp.bfloat16),
            pltpu.VMEM((4, rows, rows), jnp.float32),
            pltpu.VMEM((heads, 4, rows, rows), jnp.float32),
            pltpu.VMEM((heads, rows, half), jnp.float32),
            pltpu.VMEM((heads, 4, rows, rows), jnp.bfloat16),
            pltpu.VMEM((heads, rows, 1), jnp.float32),
            pltpu.VMEM((heads, rows, HEAD_DIM), jnp.float32),
            pltpu.VMEM((rows, GROUP_SIZE * HEAD_DIM), jnp.bfloat16),
            pltpu.VMEM((2, rows, HEAD_DIM), jnp.bfloat16),
            pltpu.VMEM((2, rows, HEAD_DIM), jnp.bfloat16),
            pltpu.VMEM((4, rows, rows), jnp.float32),
            pltpu.VMEM((GROUP_SIZE, 4, rows, rows), jnp.float32),
            pltpu.VMEM((GROUP_SIZE, 4, rows, rows), jnp.bfloat16),
            pltpu.VMEM((GROUP_SIZE, rows, HEAD_DIM), jnp.bfloat16),
            pltpu.SemaphoreType.DMA((5,)),
            pltpu.SemaphoreType.DMA((copies,)),
            pltpu.SemaphoreType.DMA((copies,)),
            pltpu.SemaphoreType.REGULAR,
        ],
        compiler_params=pltpu.CompilerParams(
            collective_id=0, has_side_effects=True, vmem_limit_bytes=56 * 1024 * 1024
        ),
        name="attend",
    )(queries, key_rows, value_rows, doc_lengths, block_owner)


def solution(mesh):
    rows = P(("seq", "ctx"), None)
    return jax.shard_map(
        functools.partial(body, mesh.shape["ctx"]),
        mesh=mesh,
        in_specs=(rows, rows, rows, P("seq"), P("seq")),
        out_specs=rows,
        check_vma=False,
    )
```

```python
import functools
import itertools
import math

import jax
import jax.numpy as jnp
from jax import lax
from jax.experimental import pallas as pl
from jax.experimental.pallas import tpu as pltpu
from jax.sharding import PartitionSpec as P

HEAD_DIM = 128
BLOCK_ROWS = 128
GROUP_SIZE = 4
NEGATIVE = -1e30
MESH = pl.DeviceIdType.MESH
EXPONENT = HEAD_DIM ** -0.5 * math.log2(math.e)

OWN, PARTNER, PREV, CROSS = range(4)


def kernel(
    devices, q_hbm, k_hbm, v_hbm, lengths_hbm, owner_hbm, out,
    lengths, owner, q, kbuf, vbuf, bias, scores, top, weights, total, acc,
    q_far, k_far, v_far, far_bias, far_scores, far_weights, o_far,
    local_sem, send_sem, recv_sem, ready,
):
    rows = q.shape[0]
    kv_heads = kbuf.shape[2] // HEAD_DIM
    lent = kv_heads - 1
    half = rows // 2
    me = lax.axis_index("ctx")
    partner = me + 1 - 2 * (me % 2)
    prev = me - 2
    cross = partner - 2
    nxt = me + 2
    has_prev = me >= 2
    has_next = me < devices - 2
    no_prev = jnp.logical_not(has_prev)
    no_next = jnp.logical_not(has_next)
    whole = jnp.logical_or(has_next, no_prev)

    barrier = pltpu.get_barrier_semaphore()

    def greet(device):
        pl.semaphore_signal(barrier, inc=1, device_id={"ctx": device}, device_id_type=MESH)

    even = me % 2 == 0
    greet(partner)
    pl.when(jnp.logical_and(has_prev, even))(lambda: greet(prev))
    pl.when(has_next)(lambda: greet(nxt))

    local = [
        pltpu.make_async_copy(k_hbm, kbuf.at[OWN], local_sem.at[0]),
        pltpu.make_async_copy(v_hbm, vbuf.at[OWN], local_sem.at[1]),
        pltpu.make_async_copy(lengths_hbm, lengths, local_sem.at[2]),
        pltpu.make_async_copy(owner_hbm, owner, local_sem.at[3]),
        pltpu.make_async_copy(q_hbm, q, local_sem.at[4]),
    ]
    for copy in local:
        copy.start()
    below = jnp.logical_and(has_next, even).astype(jnp.int32)
    pl.semaphore_wait(barrier, 1 + has_prev.astype(jnp.int32) + below)

    @pl.when(jnp.logical_and(has_prev, jnp.logical_not(even)))
    def _():
        pl.semaphore_signal(ready, inc=1, device_id={"ctx": prev}, device_id_type=MESH)


    def column(head):
        return pl.ds(head * HEAD_DIM, HEAD_DIM)

    part = [pl.ds(0, half), pl.ds(half, half)]
    every = pl.ds(0, rows)
    rest = pl.ds(0, lent * HEAD_DIM)
    indices = itertools.count()

    def remote(source, target, device):
        index = next(indices)
        return pltpu.make_async_remote_copy(
            src_ref=source, dst_ref=target, send_sem=send_sem.at[index],
            recv_sem=recv_sem.at[index], device_id={"ctx": device}, device_id_type=MESH,
        )

    def own_copy(hbm, buf, piece, columns, chunk, device):
        return remote(hbm.at[piece, columns], buf.at[chunk, piece, columns], device)

    def relay(buf, chunk, piece, columns, device):
        return remote(buf.at[chunk, piece, columns], buf.at[CROSS, piece, columns], device)

    others = range(lent)
    straight = range(lent - 1)
    k_partner = [own_copy(k_hbm, kbuf, p, rest, PARTNER, partner) for p in part]
    k_next = [own_copy(k_hbm, kbuf, p, rest, PREV, nxt) for p in part]
    lent_partner = [
        own_copy(k_hbm, kbuf, every, column(lent), PARTNER, partner),
        own_copy(v_hbm, vbuf, every, column(lent), PARTNER, partner),
    ]
    v_first_partner = own_copy(v_hbm, vbuf, part[1], rest, PARTNER, partner)
    v_first_next = own_copy(v_hbm, vbuf, part[0], rest, PREV, nxt)
    v_partner = [own_copy(v_hbm, vbuf, part[0], column(g), PARTNER, partner) for g in others]
    v_next = [own_copy(v_hbm, vbuf, part[1], column(g), PREV, nxt) for g in others]
    k_to_next = [relay(kbuf, PARTNER, part[1], column(g), nxt) for g in straight]
    k_to_partner = [relay(kbuf, PREV, part[0], column(g), partner) for g in others]
    k_late = relay(kbuf, PREV, part[1], column(lent - 1), partner)
    v_to_partner = [relay(vbuf, PREV, part[0], column(g), partner) for g in others]
    v_late = [relay(vbuf, PREV, part[1], column(g), partner) for g in others]
    far_down = [
        remote(k_hbm.at[every, column(lent)], k_far.at[0], prev),
        remote(v_hbm.at[every, column(lent)], v_far.at[0], prev),
    ]
    far_across = [
        remote(k_far.at[0], k_far.at[1], partner),
        remote(v_far.at[0], v_far.at[1], partner),
    ]
    group = range(GROUP_SIZE)
    q_down = [
        remote(q_hbm.at[every, column(lent * GROUP_SIZE + j)], q_far.at[every, column(j)], prev)
        for j in group
    ]
    o_up = [
        remote(o_far.at[j], out.at[every, column(lent * GROUP_SIZE + j)], nxt) for j in group
    ]

    def start_all(copies):
        for copy in copies:
            copy.start()

    def receive_all(copies):
        for copy in copies:
            copy.wait_recv()

    def sent_all(copies):
        for copy in copies:
            copy.wait_send()

    k_partner[1].start()
    pl.when(whole)(lambda: start_all(lent_partner))
    pl.when(jnp.logical_and(has_next, jnp.logical_not(even)))(lambda: pl.semaphore_wait(ready, 1))

    @pl.when(has_next)
    def _():
        k_next[0].start()
        k_next[1].start()
        v_first_next.start()

    @pl.when(has_prev)
    def _():
        start_all(far_down)
        start_all(q_down)

    @pl.when(no_next)
    def _():
        k_partner[0].start()
        v_first_partner.start()

    local[2].wait()
    local[3].wait()
    down = lax.broadcasted_iota(jnp.int32, (half, 1), 0)
    along = lax.broadcasted_iota(jnp.int32, (1, half), 1)

    def mask(target, chunk, querier, device):
        for i in range(2):
            places = owner[2 * querier + i] * BLOCK_ROWS + down
            end = lengths[0]
            starts = jnp.where(places >= end, end, 0)
            for d in range(1, lengths.shape[0]):
                end = end + lengths[d]
                starts = jnp.where(places >= end, end, starts)
            for j in range(2):
                keys = owner[2 * device + j] * BLOCK_ROWS + along
                allowed = (keys >= starts) & (keys <= places)
                target[chunk, pl.ds(i * half, half), pl.ds(j * half, half)] = jnp.where(
                    allowed, 0.0, NEGATIVE
                )

    mask(bias, OWN, me, me)
    mask(bias, PARTNER, me, partner)

    @pl.when(has_prev)
    def _():
        mask(bias, PREV, me, prev)
        mask(bias, CROSS, me, cross)

    @pl.when(has_next)
    def _():
        mask(far_bias, 0, nxt, me)
        mask(far_bias, 1, nxt, partner)
        mask(far_bias, 2, nxt, nxt)
        mask(far_bias, 3, nxt, partner + 2)

    def attend(queries, keys, allowed):
        s = lax.dot_general(
            queries, keys, (((1,), (1,)), ((), ())), preferred_element_type=jnp.float32
        )
        return s + allowed

    def score(chunk, first, last):
        for g in range(first, last):
            keys = kbuf[chunk, :, column(g)]
            for j in group:
                h = g * GROUP_SIZE + j
                s = attend(q[:, column(h)], keys, bias[chunk])
                scores[h, chunk] = s
                best = jnp.maximum(s[:, :half], s[:, half:])
                if chunk != OWN:
                    best = jnp.maximum(best, top[h])
                top[h] = best

    def weigh(g, chunks):
        own = vbuf[OWN, :, column(g)]
        for j in group:
            h = g * GROUP_SIZE + j
            largest = jnp.max(top[h], axis=1, keepdims=True)
            summed = jnp.zeros((rows, half), jnp.float32)
            for c in range(chunks):
                w = jnp.exp2((scores[h, c] - largest) * EXPONENT)
                summed = summed + (w[:, :half] + w[:, half:])
                weights[h, c] = w.astype(jnp.bfloat16)
            total[h] = jnp.sum(summed, axis=1, keepdims=True)
            acc[h] = jnp.dot(weights[h, OWN], own, preferred_element_type=jnp.float32)

    def mix(g):
        partners = vbuf[PARTNER, :, column(g)]
        prevs = vbuf[PREV, :, column(g)]
        for j in group:
            h = g * GROUP_SIZE + j
            acc[h] += jnp.dot(
                weights[h, PARTNER], partners, preferred_element_type=jnp.float32
            ) + jnp.dot(weights[h, PREV], prevs, preferred_element_type=jnp.float32)

    def finish(chunk, g):
        values = vbuf[chunk, :, column(g)]
        for j in group:
            h = g * GROUP_SIZE + j
            mixed = acc[h] + jnp.dot(
                weights[h, chunk], values, preferred_element_type=jnp.float32
            )
            out[:, column(h)] = (mixed * (1.0 / total[h])).astype(jnp.bfloat16)

    def far_keys(c):
        return kbuf[c, :, column(lent)] if c < 2 else k_far[c - 2]

    def far_values(c):
        return vbuf[c, :, column(lent)] if c < 2 else v_far[c - 2]

    def far_score(j):
        q_down[j].wait_recv()
        for c in range(4):
            far_scores[j, c] = attend(q_far[:, column(j)], far_keys(c), far_bias[c])

    def far_finish(j):
        best = far_scores[j, 0]
        for c in range(1, 4):
            best = jnp.maximum(best, far_scores[j, c])
        largest = jnp.max(best, axis=1, keepdims=True)
        summed = jnp.zeros((rows, half), jnp.float32)
        for c in range(4):
            w = jnp.exp2((far_scores[j, c] - largest) * EXPONENT)
            summed = summed + (w[:, :half] + w[:, half:])
            far_weights[j, c] = w.astype(jnp.bfloat16)
        mixed = jnp.dot(far_weights[j, 0], far_values(0), preferred_element_type=jnp.float32)
        for c in range(1, 4):
            mixed += jnp.dot(far_weights[j, c], far_values(c), preferred_element_type=jnp.float32)
        share = 1.0 / jnp.sum(summed, axis=1, keepdims=True)
        o_far[j] = (mixed * share).astype(jnp.bfloat16)
        o_up[j].start()

    @pl.when(has_next)
    def _():
        for down_copy, across_copy in zip(far_down, far_across):
            down_copy.wait_recv()
            across_copy.start()
        k_partner[0].start()

    k_partner[1].wait_recv()

    @pl.when(has_next)
    def _():
        start_all(k_to_next)
        start_all(v_next)
        v_first_partner.start()

    @pl.when(has_prev)
    def _():
        k_next[0].wait_recv()
        start_all(k_to_partner)
        k_next[1].wait_recv()
        k_late.start()

    start_all(v_partner)
    local[0].wait()
    local[1].wait()
    local[4].wait()
    score(OWN, 0, lent)
    pl.when(no_prev)(lambda: score(OWN, lent, kv_heads))
    pl.when(whole)(lambda: receive_all(lent_partner))

    @pl.when(has_next)
    def _():
        far_across[0].wait_recv()
        far_score(0)
        far_score(1)
        far_across[1].wait_recv()
        far_finish(0)
        far_finish(1)
        for j in group[2:]:
            far_score(j)
            far_finish(j)

    k_partner[0].wait_recv()
    score(PARTNER, 0, lent)

    @pl.when(no_prev)
    def _():
        score(PARTNER, lent, kv_heads)
        for g in range(kv_heads):
            weigh(g, 2)
        v_first_partner.wait_recv()
        for g in range(kv_heads):
            if g < lent:
                v_partner[g].wait_recv()
            finish(PARTNER, g)

    @pl.when(has_prev)
    def _():
        score(PREV, 0, lent)
        v_first_next.wait_recv()
        start_all(v_to_partner)
        for g in others:
            k_to_partner[g].wait_recv()
            (k_to_next[g] if g < lent - 1 else k_late).wait_recv()
            score(CROSS, g, g + 1)
            weigh(g, 4)
            if g == 0:
                for value, late in zip(v_next, v_late):
                    value.wait_recv()
                    late.start()
        v_first_partner.wait_recv()
        for g in others:
            v_partner[g].wait_recv()
            mix(g)
        for g in others:
            v_to_partner[g].wait_recv()
            v_late[g].wait_recv()
            finish(CROSS, g)
        receive_all(o_up)

    sent_all(k_partner + v_partner + [v_first_partner])
    pl.when(whole)(lambda: sent_all(lent_partner))
    pl.when(has_next)(
        lambda: sent_all(k_next + k_to_next + v_next + far_across + o_up + [v_first_next])
    )
    pl.when(has_prev)(
        lambda: sent_all(k_to_partner + v_to_partner + v_late + far_down + q_down + [k_late])
    )


def body(devices, queries, key_rows, value_rows, doc_lengths, block_owner):
    rows, width = queries.shape
    kv_width = key_rows.shape[1]
    heads, kv_heads = width // HEAD_DIM, kv_width // HEAD_DIM
    half = rows // 2
    copies = 8 * kv_heads + 4 + 2 * GROUP_SIZE
    return pl.pallas_call(
        functools.partial(kernel, devices),
        out_shape=pltpu.VMEM((rows, width), jnp.bfloat16),
        in_specs=[pl.BlockSpec(memory_space=pl.ANY)] * 5,
        out_specs=pl.BlockSpec(memory_space=pltpu.VMEM),
        scratch_shapes=[
            pltpu.SMEM(doc_lengths.shape, jnp.int32),
            pltpu.SMEM(block_owner.shape, jnp.int32),
            pltpu.VMEM((rows, width), jnp.bfloat16),
            pltpu.VMEM((4, rows, kv_width), jnp.bfloat16),
            pltpu.VMEM((4, rows, kv_width), jnp.bfloat16),
            pltpu.VMEM((4, rows, rows), jnp.float32),
            pltpu.VMEM((heads, 4, rows, rows), jnp.float32),
            pltpu.VMEM((heads, rows, half), jnp.float32),
            pltpu.VMEM((heads, 4, rows, rows), jnp.bfloat16),
            pltpu.VMEM((heads, rows, 1), jnp.float32),
            pltpu.VMEM((heads, rows, HEAD_DIM), jnp.float32),
            pltpu.VMEM((rows, GROUP_SIZE * HEAD_DIM), jnp.bfloat16),
            pltpu.VMEM((2, rows, HEAD_DIM), jnp.bfloat16),
            pltpu.VMEM((2, rows, HEAD_DIM), jnp.bfloat16),
            pltpu.VMEM((4, rows, rows), jnp.float32),
            pltpu.VMEM((GROUP_SIZE, 4, rows, rows), jnp.float32),
            pltpu.VMEM((GROUP_SIZE, 4, rows, rows), jnp.bfloat16),
            pltpu.VMEM((GROUP_SIZE, rows, HEAD_DIM), jnp.bfloat16),
            pltpu.SemaphoreType.DMA((5,)),
            pltpu.SemaphoreType.DMA((copies,)),
            pltpu.SemaphoreType.DMA((copies,)),
            pltpu.SemaphoreType.REGULAR,
        ],
        compiler_params=pltpu.CompilerParams(
            collective_id=0, has_side_effects=True, vmem_limit_bytes=56 * 1024 * 1024
        ),
        name="attend",
    )(queries, key_rows, value_rows, doc_lengths, block_owner)


def solution(mesh):
    rows = P(("seq", "ctx"), None)
    return jax.shard_map(
        functools.partial(body, mesh.shape["ctx"]),
        mesh=mesh,
        in_specs=(rows, rows, rows, P("seq"), P("seq")),
        out_specs=rows,
        check_vma=False,
    )
```

```python
import functools
import itertools
import math

import jax
import jax.numpy as jnp
from jax import lax
from jax.experimental import pallas as pl
from jax.experimental.pallas import tpu as pltpu
from jax.sharding import PartitionSpec as P

HEAD_DIM = 128
BLOCK_ROWS = 128
GROUP_SIZE = 4
NEGATIVE = -1e30
MESH = pl.DeviceIdType.MESH
EXPONENT = HEAD_DIM ** -0.5 * math.log2(math.e)

OWN, PARTNER, PREV, CROSS = range(4)


def kernel(
    devices, q_hbm, k_hbm, v_hbm, lengths_hbm, owner_hbm, out,
    lengths, owner, q, kbuf, vbuf, bias, scores, top, weights, total, acc,
    q_far, k_far, v_far, far_bias, far_scores, far_weights, o_far,
    local_sem, send_sem, recv_sem, ready,
):
    rows = q.shape[0]
    kv_heads = kbuf.shape[2] // HEAD_DIM
    lent = kv_heads - 1
    half = rows // 2
    me = lax.axis_index("ctx")
    partner = me + 1 - 2 * (me % 2)
    prev = me - 2
    cross = partner - 2
    nxt = me + 2
    has_prev = me >= 2
    has_next = me < devices - 2
    no_prev = jnp.logical_not(has_prev)
    no_next = jnp.logical_not(has_next)
    whole = jnp.logical_or(has_next, no_prev)

    barrier = pltpu.get_barrier_semaphore()

    def greet(device):
        pl.semaphore_signal(barrier, inc=1, device_id={"ctx": device}, device_id_type=MESH)

    even = me % 2 == 0
    greet(partner)
    pl.when(jnp.logical_and(has_prev, even))(lambda: greet(prev))
    pl.when(has_next)(lambda: greet(nxt))

    local = [
        pltpu.make_async_copy(k_hbm, kbuf.at[OWN], local_sem.at[0]),
        pltpu.make_async_copy(v_hbm, vbuf.at[OWN], local_sem.at[1]),
        pltpu.make_async_copy(lengths_hbm, lengths, local_sem.at[2]),
        pltpu.make_async_copy(owner_hbm, owner, local_sem.at[3]),
        pltpu.make_async_copy(q_hbm, q, local_sem.at[4]),
    ]
    for copy in local:
        copy.start()
    below = jnp.logical_and(has_next, even).astype(jnp.int32)
    pl.semaphore_wait(barrier, 1 + has_prev.astype(jnp.int32) + below)

    @pl.when(jnp.logical_and(has_prev, jnp.logical_not(even)))
    def _():
        pl.semaphore_signal(ready, inc=1, device_id={"ctx": prev}, device_id_type=MESH)


    def column(head):
        return pl.ds(head * HEAD_DIM, HEAD_DIM)

    part = [pl.ds(0, half), pl.ds(half, half)]
    every = pl.ds(0, rows)
    rest = pl.ds(0, lent * HEAD_DIM)
    indices = itertools.count()

    def remote(source, target, device):
        index = next(indices)
        return pltpu.make_async_remote_copy(
            src_ref=source, dst_ref=target, send_sem=send_sem.at[index],
            recv_sem=recv_sem.at[index], device_id={"ctx": device}, device_id_type=MESH,
        )

    def own_copy(hbm, buf, piece, columns, chunk, device):
        return remote(hbm.at[piece, columns], buf.at[chunk, piece, columns], device)

    def relay(buf, chunk, piece, columns, device):
        return remote(buf.at[chunk, piece, columns], buf.at[CROSS, piece, columns], device)

    others = range(lent)
    straight = range(lent - 1)
    k_partner = [own_copy(k_hbm, kbuf, p, rest, PARTNER, partner) for p in part]
    k_next = [own_copy(k_hbm, kbuf, p, rest, PREV, nxt) for p in part]
    lent_partner = [
        own_copy(k_hbm, kbuf, every, column(lent), PARTNER, partner),
        own_copy(v_hbm, vbuf, every, column(lent), PARTNER, partner),
    ]
    v_first_partner = own_copy(v_hbm, vbuf, part[1], rest, PARTNER, partner)
    v_first_next = own_copy(v_hbm, vbuf, part[0], rest, PREV, nxt)
    v_partner = [own_copy(v_hbm, vbuf, part[0], rest, PARTNER, partner)]
    v_next = [own_copy(v_hbm, vbuf, part[1], column(g), PREV, nxt) for g in others]
    k_to_next = [relay(kbuf, PARTNER, part[1], column(g), nxt) for g in straight]
    k_to_partner = [relay(kbuf, PREV, part[0], column(g), partner) for g in others]
    k_late = relay(kbuf, PREV, part[1], column(lent - 1), partner)
    v_to_partner = [relay(vbuf, PREV, part[0], column(g), partner) for g in others]
    v_late = [relay(vbuf, PREV, part[1], column(g), partner) for g in others]
    far_down = [
        remote(k_hbm.at[every, column(lent)], k_far.at[0], prev),
        remote(v_hbm.at[every, column(lent)], v_far.at[0], prev),
    ]
    far_across = [
        remote(k_far.at[0], k_far.at[1], partner),
        remote(v_far.at[0], v_far.at[1], partner),
    ]
    group = range(GROUP_SIZE)
    q_down = [
        remote(q_hbm.at[every, column(lent * GROUP_SIZE + j)], q_far.at[every, column(j)], prev)
        for j in group
    ]
    o_up = [
        remote(o_far.at[j], out.at[every, column(lent * GROUP_SIZE + j)], nxt) for j in group
    ]

    def start_all(copies):
        for copy in copies:
            copy.start()

    def receive_all(copies):
        for copy in copies:
            copy.wait_recv()

    def sent_all(copies):
        for copy in copies:
            copy.wait_send()

    k_partner[1].start()
    pl.when(whole)(lambda: start_all(lent_partner))
    pl.when(jnp.logical_and(has_next, jnp.logical_not(even)))(lambda: pl.semaphore_wait(ready, 1))

    @pl.when(has_next)
    def _():
        k_next[0].start()
        k_next[1].start()
        v_first_next.start()

    @pl.when(has_prev)
    def _():
        start_all(far_down)
        start_all(q_down)

    @pl.when(no_next)
    def _():
        k_partner[0].start()
        v_first_partner.start()

    local[2].wait()
    local[3].wait()
    down = lax.broadcasted_iota(jnp.int32, (half, 1), 0)
    along = lax.broadcasted_iota(jnp.int32, (1, half), 1)

    def mask(target, chunk, querier, device):
        for i in range(2):
            places = owner[2 * querier + i] * BLOCK_ROWS + down
            end = lengths[0]
            starts = jnp.where(places >= end, end, 0)
            for d in range(1, lengths.shape[0]):
                end = end + lengths[d]
                starts = jnp.where(places >= end, end, starts)
            for j in range(2):
                keys = owner[2 * device + j] * BLOCK_ROWS + along
                allowed = (keys >= starts) & (keys <= places)
                target[chunk, pl.ds(i * half, half), pl.ds(j * half, half)] = jnp.where(
                    allowed, 0.0, NEGATIVE
                )

    mask(bias, OWN, me, me)
    mask(bias, PARTNER, me, partner)

    @pl.when(has_prev)
    def _():
        mask(bias, PREV, me, prev)
        mask(bias, CROSS, me, cross)

    @pl.when(has_next)
    def _():
        mask(far_bias, 0, nxt, me)
        mask(far_bias, 1, nxt, partner)
        mask(far_bias, 2, nxt, nxt)
        mask(far_bias, 3, nxt, partner + 2)

    def attend(queries, keys, allowed):
        s = lax.dot_general(
            queries, keys, (((1,), (1,)), ((), ())), preferred_element_type=jnp.float32
        )
        return s + allowed

    def score(chunk, first, last):
        for g in range(first, last):
            keys = kbuf[chunk, :, column(g)]
            for j in group:
                h = g * GROUP_SIZE + j
                s = attend(q[:, column(h)], keys, bias[chunk])
                scores[h, chunk] = s
                best = jnp.maximum(s[:, :half], s[:, half:])
                if chunk != OWN:
                    best = jnp.maximum(best, top[h])
                top[h] = best

    def weigh(g, chunks):
        own = vbuf[OWN, :, column(g)]
        for j in group:
            h = g * GROUP_SIZE + j
            largest = jnp.max(top[h], axis=1, keepdims=True)
            summed = jnp.zeros((rows, half), jnp.float32)
            for c in range(chunks):
                w = jnp.exp2((scores[h, c] - largest) * EXPONENT)
                summed = summed + (w[:, :half] + w[:, half:])
                weights[h, c] = w.astype(jnp.bfloat16)
            total[h] = jnp.sum(summed, axis=1, keepdims=True)
            acc[h] = jnp.dot(weights[h, OWN], own, preferred_element_type=jnp.float32)

    def mix(g):
        partners = vbuf[PARTNER, :, column(g)]
        prevs = vbuf[PREV, :, column(g)]
        for j in group:
            h = g * GROUP_SIZE + j
            acc[h] += jnp.dot(
                weights[h, PARTNER], partners, preferred_element_type=jnp.float32
            ) + jnp.dot(weights[h, PREV], prevs, preferred_element_type=jnp.float32)

    def finish(chunk, g):
        values = vbuf[chunk, :, column(g)]
        for j in group:
            h = g * GROUP_SIZE + j
            mixed = acc[h] + jnp.dot(
                weights[h, chunk], values, preferred_element_type=jnp.float32
            )
            out[:, column(h)] = (mixed * (1.0 / total[h])).astype(jnp.bfloat16)

    def far_keys(c):
        return kbuf[c, :, column(lent)] if c < 2 else k_far[c - 2]

    def far_values(c):
        return vbuf[c, :, column(lent)] if c < 2 else v_far[c - 2]

    def far_score(j):
        q_down[j].wait_recv()
        for c in range(4):
            far_scores[j, c] = attend(q_far[:, column(j)], far_keys(c), far_bias[c])

    def far_finish(j):
        best = far_scores[j, 0]
        for c in range(1, 4):
            best = jnp.maximum(best, far_scores[j, c])
        largest = jnp.max(best, axis=1, keepdims=True)
        summed = jnp.zeros((rows, half), jnp.float32)
        for c in range(4):
            w = jnp.exp2((far_scores[j, c] - largest) * EXPONENT)
            summed = summed + (w[:, :half] + w[:, half:])
            far_weights[j, c] = w.astype(jnp.bfloat16)
        mixed = jnp.dot(far_weights[j, 0], far_values(0), preferred_element_type=jnp.float32)
        for c in range(1, 4):
            mixed += jnp.dot(far_weights[j, c], far_values(c), preferred_element_type=jnp.float32)
        share = 1.0 / jnp.sum(summed, axis=1, keepdims=True)
        o_far[j] = (mixed * share).astype(jnp.bfloat16)
        o_up[j].start()

    @pl.when(has_next)
    def _():
        for down_copy, across_copy in zip(far_down, far_across):
            down_copy.wait_recv()
            across_copy.start()
        k_partner[0].start()

    k_partner[1].wait_recv()

    @pl.when(has_next)
    def _():
        start_all(k_to_next)
        start_all(v_next)
        v_first_partner.start()

    @pl.when(has_prev)
    def _():
        k_next[0].wait_recv()
        start_all(k_to_partner)
        k_next[1].wait_recv()
        k_late.start()

    start_all(v_partner)
    local[0].wait()
    local[1].wait()
    local[4].wait()
    score(OWN, 0, lent)
    pl.when(no_prev)(lambda: score(OWN, lent, kv_heads))
    pl.when(whole)(lambda: receive_all(lent_partner))

    @pl.when(has_next)
    def _():
        far_across[0].wait_recv()
        far_score(0)
        far_score(1)
        far_across[1].wait_recv()
        far_finish(0)
        far_finish(1)
        for j in group[2:]:
            far_score(j)
            far_finish(j)

    k_partner[0].wait_recv()
    score(PARTNER, 0, lent)

    @pl.when(no_prev)
    def _():
        score(PARTNER, lent, kv_heads)
        for g in range(kv_heads):
            weigh(g, 2)
        v_first_partner.wait_recv()
        for g in range(kv_heads):
            if g == 0:
                v_partner[0].wait_recv()
            finish(PARTNER, g)

    @pl.when(has_prev)
    def _():
        score(PREV, 0, lent)
        v_first_next.wait_recv()
        start_all(v_to_partner)
        for g in others:
            k_to_partner[g].wait_recv()
            (k_to_next[g] if g < lent - 1 else k_late).wait_recv()
            score(CROSS, g, g + 1)
            weigh(g, 4)
            if g == 0:
                for value, late in zip(v_next, v_late):
                    value.wait_recv()
                    late.start()
        v_first_partner.wait_recv()
        for g in others:
            if g == 0:
                v_partner[0].wait_recv()
            mix(g)
        for g in others:
            v_to_partner[g].wait_recv()
            v_late[g].wait_recv()
            finish(CROSS, g)
        receive_all(o_up)

    sent_all(k_partner + v_partner + [v_first_partner])
    pl.when(whole)(lambda: sent_all(lent_partner))
    pl.when(has_next)(
        lambda: sent_all(k_next + k_to_next + v_next + far_across + o_up + [v_first_next])
    )
    pl.when(has_prev)(
        lambda: sent_all(k_to_partner + v_to_partner + v_late + far_down + q_down + [k_late])
    )


def body(devices, queries, key_rows, value_rows, doc_lengths, block_owner):
    rows, width = queries.shape
    kv_width = key_rows.shape[1]
    heads, kv_heads = width // HEAD_DIM, kv_width // HEAD_DIM
    half = rows // 2
    copies = 8 * kv_heads + 4 + 2 * GROUP_SIZE
    return pl.pallas_call(
        functools.partial(kernel, devices),
        out_shape=pltpu.VMEM((rows, width), jnp.bfloat16),
        in_specs=[pl.BlockSpec(memory_space=pl.ANY)] * 5,
        out_specs=pl.BlockSpec(memory_space=pltpu.VMEM),
        scratch_shapes=[
            pltpu.SMEM(doc_lengths.shape, jnp.int32),
            pltpu.SMEM(block_owner.shape, jnp.int32),
            pltpu.VMEM((rows, width), jnp.bfloat16),
            pltpu.VMEM((4, rows, kv_width), jnp.bfloat16),
            pltpu.VMEM((4, rows, kv_width), jnp.bfloat16),
            pltpu.VMEM((4, rows, rows), jnp.float32),
            pltpu.VMEM((heads, 4, rows, rows), jnp.float32),
            pltpu.VMEM((heads, rows, half), jnp.float32),
            pltpu.VMEM((heads, 4, rows, rows), jnp.bfloat16),
            pltpu.VMEM((heads, rows, 1), jnp.float32),
            pltpu.VMEM((heads, rows, HEAD_DIM), jnp.float32),
            pltpu.VMEM((rows, GROUP_SIZE * HEAD_DIM), jnp.bfloat16),
            pltpu.VMEM((2, rows, HEAD_DIM), jnp.bfloat16),
            pltpu.VMEM((2, rows, HEAD_DIM), jnp.bfloat16),
            pltpu.VMEM((4, rows, rows), jnp.float32),
            pltpu.VMEM((GROUP_SIZE, 4, rows, rows), jnp.float32),
            pltpu.VMEM((GROUP_SIZE, 4, rows, rows), jnp.bfloat16),
            pltpu.VMEM((GROUP_SIZE, rows, HEAD_DIM), jnp.bfloat16),
            pltpu.SemaphoreType.DMA((5,)),
            pltpu.SemaphoreType.DMA((copies,)),
            pltpu.SemaphoreType.DMA((copies,)),
            pltpu.SemaphoreType.REGULAR,
        ],
        compiler_params=pltpu.CompilerParams(
            collective_id=0, has_side_effects=True, vmem_limit_bytes=56 * 1024 * 1024
        ),
        name="attend",
    )(queries, key_rows, value_rows, doc_lengths, block_owner)


def solution(mesh):
    rows = P(("seq", "ctx"), None)
    return jax.shard_map(
        functools.partial(body, mesh.shape["ctx"]),
        mesh=mesh,
        in_specs=(rows, rows, rows, P("seq"), P("seq")),
        out_specs=rows,
        check_vma=False,
    )
```

```python
import functools
import itertools
import math

import jax
import jax.numpy as jnp
from jax import lax
from jax.experimental import pallas as pl
from jax.experimental.pallas import tpu as pltpu
from jax.sharding import PartitionSpec as P

HEAD_DIM = 128
BLOCK_ROWS = 128
GROUP_SIZE = 4
NEGATIVE = -1e30
MESH = pl.DeviceIdType.MESH
EXPONENT = HEAD_DIM ** -0.5 * math.log2(math.e)

OWN, PARTNER, PREV, CROSS = range(4)


def kernel(
    devices, q_hbm, k_hbm, v_hbm, lengths_hbm, owner_hbm, out,
    lengths, owner, q, kbuf, vbuf, bias, scores, top, weights, total, acc,
    q_far, k_far, v_far, far_bias, far_scores, far_weights, o_far,
    local_sem, send_sem, recv_sem, ready,
):
    rows = q.shape[0]
    kv_heads = kbuf.shape[2] // HEAD_DIM
    lent = kv_heads - 1
    half = rows // 2
    me = lax.axis_index("ctx")
    partner = me + 1 - 2 * (me % 2)
    prev = me - 2
    cross = partner - 2
    nxt = me + 2
    has_prev = me >= 2
    has_next = me < devices - 2
    no_prev = jnp.logical_not(has_prev)
    no_next = jnp.logical_not(has_next)
    whole = jnp.logical_or(has_next, no_prev)

    barrier = pltpu.get_barrier_semaphore()

    def greet(device):
        pl.semaphore_signal(barrier, inc=1, device_id={"ctx": device}, device_id_type=MESH)

    even = me % 2 == 0
    second = lax.axis_index("seq") % 2 == 1
    first = jnp.logical_not(second)
    greet(partner)
    pl.when(jnp.logical_and(has_prev, even))(lambda: greet(prev))
    pl.when(has_next)(lambda: greet(nxt))

    local = [
        pltpu.make_async_copy(k_hbm, kbuf.at[OWN], local_sem.at[0]),
        pltpu.make_async_copy(v_hbm, vbuf.at[OWN], local_sem.at[1]),
        pltpu.make_async_copy(lengths_hbm, lengths, local_sem.at[2]),
        pltpu.make_async_copy(owner_hbm, owner, local_sem.at[3]),
        pltpu.make_async_copy(q_hbm, q, local_sem.at[4]),
    ]
    for copy in local:
        copy.start()
    below = jnp.logical_and(has_next, even).astype(jnp.int32)
    pl.semaphore_wait(barrier, 1 + has_prev.astype(jnp.int32) + below)

    @pl.when(jnp.logical_and(has_prev, jnp.logical_not(even)))
    def _():
        pl.semaphore_signal(ready, inc=1, device_id={"ctx": prev}, device_id_type=MESH)


    def column(head):
        return pl.ds(head * HEAD_DIM, HEAD_DIM)

    part = [pl.ds(0, half), pl.ds(half, half)]
    every = pl.ds(0, rows)
    rest = pl.ds(0, lent * HEAD_DIM)
    indices = itertools.count()

    def remote(source, target, device):
        index = next(indices)
        return pltpu.make_async_remote_copy(
            src_ref=source, dst_ref=target, send_sem=send_sem.at[index],
            recv_sem=recv_sem.at[index], device_id={"ctx": device}, device_id_type=MESH,
        )

    def own_copy(hbm, buf, piece, columns, chunk, device):
        return remote(hbm.at[piece, columns], buf.at[chunk, piece, columns], device)

    def relay(buf, chunk, piece, columns, device):
        return remote(buf.at[chunk, piece, columns], buf.at[CROSS, piece, columns], device)

    others = range(lent)
    straight = range(lent - 1)
    k_partner = [own_copy(k_hbm, kbuf, p, rest, PARTNER, partner) for p in part]
    k_next = [own_copy(k_hbm, kbuf, p, rest, PREV, nxt) for p in part]
    lent_partner = [
        own_copy(k_hbm, kbuf, every, column(lent), PARTNER, partner),
        own_copy(v_hbm, vbuf, every, column(lent), PARTNER, partner),
    ]
    v_first_partner = own_copy(v_hbm, vbuf, part[1], rest, PARTNER, partner)
    v_first_next = own_copy(v_hbm, vbuf, part[0], rest, PREV, nxt)
    v_partner = [own_copy(v_hbm, vbuf, part[0], rest, PARTNER, partner)]
    v_next = [own_copy(v_hbm, vbuf, part[1], column(g), PREV, nxt) for g in others]
    k_to_next = [relay(kbuf, PARTNER, part[1], column(g), nxt) for g in straight]
    k_to_partner = [relay(kbuf, PREV, part[0], column(g), partner) for g in others]
    k_late = relay(kbuf, PREV, part[1], column(lent - 1), partner)
    v_to_partner = [relay(vbuf, PREV, part[0], column(g), partner) for g in others]
    v_late = [relay(vbuf, PREV, part[1], column(g), partner) for g in others]
    far_down = [
        remote(k_hbm.at[every, column(lent)], k_far.at[0], prev),
        remote(v_hbm.at[every, column(lent)], v_far.at[0], prev),
    ]
    far_across = [
        remote(k_far.at[0], k_far.at[1], partner),
        remote(v_far.at[0], v_far.at[1], partner),
    ]
    group = range(GROUP_SIZE)
    q_down = [
        remote(q_hbm.at[every, column(lent * GROUP_SIZE + j)], q_far.at[every, column(j)], prev)
        for j in group
    ]
    o_up = [
        remote(o_far.at[j], out.at[every, column(lent * GROUP_SIZE + j)], nxt) for j in group
    ]

    def start_all(copies):
        for copy in copies:
            copy.start()

    def receive_all(copies):
        for copy in copies:
            copy.wait_recv()

    def sent_all(copies):
        for copy in copies:
            copy.wait_send()

    k_partner[1].start()
    pl.when(whole)(lambda: start_all(lent_partner))
    pl.when(jnp.logical_and(has_next, jnp.logical_not(even)))(lambda: pl.semaphore_wait(ready, 1))

    @pl.when(has_next)
    def _():
        k_next[0].start()
        k_next[1].start()
        v_first_next.start()

    @pl.when(has_prev)
    def _():
        start_all(far_down)
        start_all(q_down)

    @pl.when(no_next)
    def _():
        k_partner[0].start()
        v_first_partner.start()

    local[2].wait()
    local[3].wait()
    down = lax.broadcasted_iota(jnp.int32, (half, 1), 0)
    along = lax.broadcasted_iota(jnp.int32, (1, half), 1)

    def mask(target, chunk, querier, device):
        for i in range(2):
            places = owner[2 * querier + i] * BLOCK_ROWS + down
            end = lengths[0]
            starts = jnp.where(places >= end, end, 0)
            for d in range(1, lengths.shape[0]):
                end = end + lengths[d]
                starts = jnp.where(places >= end, end, starts)
            for j in range(2):
                keys = owner[2 * device + j] * BLOCK_ROWS + along
                allowed = (keys >= starts) & (keys <= places)
                target[chunk, pl.ds(i * half, half), pl.ds(j * half, half)] = jnp.where(
                    allowed, 0.0, NEGATIVE
                )

    mask(bias, OWN, me, me)
    mask(bias, PARTNER, me, partner)

    @pl.when(has_prev)
    def _():
        mask(bias, PREV, me, prev)
        mask(bias, CROSS, me, cross)

    @pl.when(has_next)
    def _():
        mask(far_bias, 0, nxt, me)
        mask(far_bias, 1, nxt, partner)
        mask(far_bias, 2, nxt, nxt)
        mask(far_bias, 3, nxt, partner + 2)

    def attend(queries, keys, allowed):
        s = lax.dot_general(
            queries, keys, (((1,), (1,)), ((), ())), preferred_element_type=jnp.float32
        )
        return s + allowed

    def score(chunk, first, last):
        for g in range(first, last):
            keys = kbuf[chunk, :, column(g)]
            for j in group:
                h = g * GROUP_SIZE + j
                s = attend(q[:, column(h)], keys, bias[chunk])
                scores[h, chunk] = s
                best = jnp.maximum(s[:, :half], s[:, half:])
                if chunk != OWN:
                    best = jnp.maximum(best, top[h])
                top[h] = best

    def weigh(g, chunks):
        own = vbuf[OWN, :, column(g)]
        for j in group:
            h = g * GROUP_SIZE + j
            largest = jnp.max(top[h], axis=1, keepdims=True)
            summed = jnp.zeros((rows, half), jnp.float32)
            for c in range(chunks):
                w = jnp.exp2((scores[h, c] - largest) * EXPONENT)
                summed = summed + (w[:, :half] + w[:, half:])
                weights[h, c] = w.astype(jnp.bfloat16)
            total[h] = jnp.sum(summed, axis=1, keepdims=True)
            acc[h] = jnp.dot(weights[h, OWN], own, preferred_element_type=jnp.float32)

    def mix(g):
        partners = vbuf[PARTNER, :, column(g)]
        prevs = vbuf[PREV, :, column(g)]
        for j in group:
            h = g * GROUP_SIZE + j
            acc[h] += jnp.dot(
                weights[h, PARTNER], partners, preferred_element_type=jnp.float32
            ) + jnp.dot(weights[h, PREV], prevs, preferred_element_type=jnp.float32)

    def finish(chunk, g):
        values = vbuf[chunk, :, column(g)]
        for j in group:
            h = g * GROUP_SIZE + j
            mixed = acc[h] + jnp.dot(
                weights[h, chunk], values, preferred_element_type=jnp.float32
            )
            out[:, column(h)] = (mixed * (1.0 / total[h])).astype(jnp.bfloat16)

    def far_keys(c):
        return kbuf[c, :, column(lent)] if c < 2 else k_far[c - 2]

    def far_values(c):
        return vbuf[c, :, column(lent)] if c < 2 else v_far[c - 2]

    def far_score(j):
        q_down[j].wait_recv()
        for c in range(4):
            far_scores[j, c] = attend(q_far[:, column(j)], far_keys(c), far_bias[c])

    def far_finish(j):
        best = far_scores[j, 0]
        for c in range(1, 4):
            best = jnp.maximum(best, far_scores[j, c])
        largest = jnp.max(best, axis=1, keepdims=True)
        summed = jnp.zeros((rows, half), jnp.float32)
        for c in range(4):
            w = jnp.exp2((far_scores[j, c] - largest) * EXPONENT)
            summed = summed + (w[:, :half] + w[:, half:])
            far_weights[j, c] = w.astype(jnp.bfloat16)
        mixed = jnp.dot(far_weights[j, 0], far_values(0), preferred_element_type=jnp.float32)
        for c in range(1, 4):
            mixed += jnp.dot(far_weights[j, c], far_values(c), preferred_element_type=jnp.float32)
        share = 1.0 / jnp.sum(summed, axis=1, keepdims=True)
        o_far[j] = (mixed * share).astype(jnp.bfloat16)
        o_up[j].start()

    @pl.when(has_next)
    def _():
        for down_copy, across_copy in zip(far_down, far_across):
            down_copy.wait_recv()
            across_copy.start()
        k_partner[0].start()

    k_partner[1].wait_recv()

    @pl.when(has_next)
    def _():
        start_all(k_to_next)
        start_all(v_next)
        v_first_partner.start()

    @pl.when(has_prev)
    def _():
        k_next[0].wait_recv()
        start_all(k_to_partner)
        k_next[1].wait_recv()
        k_late.start()

    pl.when(first)(lambda: start_all(v_partner))
    local[0].wait()
    local[1].wait()
    local[4].wait()
    score(OWN, 0, lent)
    pl.when(no_prev)(lambda: score(OWN, lent, kv_heads))
    pl.when(whole)(lambda: receive_all(lent_partner))

    @pl.when(has_next)
    def _():
        far_across[0].wait_recv()
        far_score(0)
        far_score(1)
        far_across[1].wait_recv()
        far_finish(0)
        far_finish(1)
        for j in group[2:]:
            far_score(j)
            far_finish(j)

    k_partner[0].wait_recv()
    score(PARTNER, 0, lent)
    pl.when(second)(lambda: start_all(v_partner))

    @pl.when(no_prev)
    def _():
        score(PARTNER, lent, kv_heads)
        for g in range(kv_heads):
            weigh(g, 2)
        v_first_partner.wait_recv()
        for g in range(kv_heads):
            if g == 0:
                v_partner[0].wait_recv()
            finish(PARTNER, g)

    @pl.when(has_prev)
    def _():
        score(PREV, 0, lent)
        v_first_next.wait_recv()
        start_all(v_to_partner)
        for g in others:
            k_to_partner[g].wait_recv()
            (k_to_next[g] if g < lent - 1 else k_late).wait_recv()
            score(CROSS, g, g + 1)
            weigh(g, 4)
            if g == 0:
                for value, late in zip(v_next, v_late):
                    value.wait_recv()
                    late.start()
        v_first_partner.wait_recv()
        for g in others:
            if g == 0:
                v_partner[0].wait_recv()
            mix(g)
        for g in others:
            v_to_partner[g].wait_recv()
            v_late[g].wait_recv()
            finish(CROSS, g)
        receive_all(o_up)

    sent_all(k_partner + v_partner + [v_first_partner])
    pl.when(whole)(lambda: sent_all(lent_partner))
    pl.when(has_next)(
        lambda: sent_all(k_next + k_to_next + v_next + far_across + o_up + [v_first_next])
    )
    pl.when(has_prev)(
        lambda: sent_all(k_to_partner + v_to_partner + v_late + far_down + q_down + [k_late])
    )


def body(devices, queries, key_rows, value_rows, doc_lengths, block_owner):
    rows, width = queries.shape
    kv_width = key_rows.shape[1]
    heads, kv_heads = width // HEAD_DIM, kv_width // HEAD_DIM
    half = rows // 2
    copies = 8 * kv_heads + 4 + 2 * GROUP_SIZE
    return pl.pallas_call(
        functools.partial(kernel, devices),
        out_shape=pltpu.VMEM((rows, width), jnp.bfloat16),
        in_specs=[pl.BlockSpec(memory_space=pl.ANY)] * 5,
        out_specs=pl.BlockSpec(memory_space=pltpu.VMEM),
        scratch_shapes=[
            pltpu.SMEM(doc_lengths.shape, jnp.int32),
            pltpu.SMEM(block_owner.shape, jnp.int32),
            pltpu.VMEM((rows, width), jnp.bfloat16),
            pltpu.VMEM((4, rows, kv_width), jnp.bfloat16),
            pltpu.VMEM((4, rows, kv_width), jnp.bfloat16),
            pltpu.VMEM((4, rows, rows), jnp.float32),
            pltpu.VMEM((heads, 4, rows, rows), jnp.float32),
            pltpu.VMEM((heads, rows, half), jnp.float32),
            pltpu.VMEM((heads, 4, rows, rows), jnp.bfloat16),
            pltpu.VMEM((heads, rows, 1), jnp.float32),
            pltpu.VMEM((heads, rows, HEAD_DIM), jnp.float32),
            pltpu.VMEM((rows, GROUP_SIZE * HEAD_DIM), jnp.bfloat16),
            pltpu.VMEM((2, rows, HEAD_DIM), jnp.bfloat16),
            pltpu.VMEM((2, rows, HEAD_DIM), jnp.bfloat16),
            pltpu.VMEM((4, rows, rows), jnp.float32),
            pltpu.VMEM((GROUP_SIZE, 4, rows, rows), jnp.float32),
            pltpu.VMEM((GROUP_SIZE, 4, rows, rows), jnp.bfloat16),
            pltpu.VMEM((GROUP_SIZE, rows, HEAD_DIM), jnp.bfloat16),
            pltpu.SemaphoreType.DMA((5,)),
            pltpu.SemaphoreType.DMA((copies,)),
            pltpu.SemaphoreType.DMA((copies,)),
            pltpu.SemaphoreType.REGULAR,
        ],
        compiler_params=pltpu.CompilerParams(
            collective_id=0, has_side_effects=True, vmem_limit_bytes=56 * 1024 * 1024
        ),
        name="attend",
    )(queries, key_rows, value_rows, doc_lengths, block_owner)


def solution(mesh):
    rows = P(("seq", "ctx"), None)
    return jax.shard_map(
        functools.partial(body, mesh.shape["ctx"]),
        mesh=mesh,
        in_specs=(rows, rows, rows, P("seq"), P("seq")),
        out_specs=rows,
        check_vma=False,
    )
```
